32 devices in a mesh: data: 32 (over z, y, x, core).
Axes of the slice: x: 2, y: 2, z: 4, core: 2. Of those that a mesh axis runs over, the one named last changes fastest.
Arguments:
- tokens: bfloat16 [262144, 256], P('data')
- out_grad: bfloat16 [262144, 256], P('data')
- w_up: bfloat16 [2, 256, 1024], replicated
- w_down: bfloat16 [2, 1024, 256], replicated
- a_up_old: float32 [2, 256, 256], replicated
- s_up_old: float32 [2, 1024, 1024], replicated
- a_down_old: float32 [2, 1024, 1024], replicated
- s_down_old: float32 [2, 256, 256], replicated
- a_up_inv: float32 [2, 256, 256], replicated
- s_up_inv: float32 [2, 1024, 1024], replicated
- a_down_inv: float32 [2, 1024, 1024], replicated
- s_down_inv: float32 [2, 256, 256], replicated
- factor_decay: float32 [], replicated
Outputs:
- output 1: float32 [2, 256, 1024], replicated
- output 2: float32 [2, 1024, 256], replicated
- output 3: float32 [2, 256, 256], replicated
- output 4: float32 [2, 1024, 1024], replicated
- output 5: float32 [2, 1024, 1024], replicated
- output 6: float32 [2, 256, 256], replicated
All inputs are finite; a program needn't handle non-finite values.
Results may differ from the reference program's by a relative error of at most 0.00171367.
Values are sent between devices in bfloat16 or wider.
A program may use at most 1 GiB of HBM per device.

```python
import math
import jax
import jax.numpy as jnp
from jax import lax

D = 256
FF = 1024
TOK_DEV = 8192
SHARDS = 32
BLOCKS = 2


def gelu_fn(pre_act):
    return jax.nn.gelu(pre_act, approximate=True)


def spd_draw(rng_key, width, diag_low, diag_high):
    key_diag, key_low = jax.random.split(rng_key)
    diag_part = jax.random.uniform(key_diag, (BLOCKS, width), jnp.float32, diag_low, diag_high)
    low_rank = jax.random.normal(key_low, (BLOCKS, width, 64), jnp.float32)
    outer_part = jnp.einsum("bik,bjk->bij", low_rank, low_rank) / math.sqrt(width * 64.0)
    return outer_part + diag_part[:, :, None] * jnp.eye(width, dtype=jnp.float32)[None]


def shifted_rows(key_scale, key_shift, key_noise):
    row_scale = jnp.exp(1.5 * jax.random.uniform(key_scale, (SHARDS, 1, 1), jnp.float32, -1.0, 1.0))
    row_shift = 0.7 * jax.random.normal(key_shift, (SHARDS, 1, D), jnp.float32)
    row_noise = jax.random.normal(key_noise, (SHARDS, TOK_DEV, D), jnp.float32)
    return (row_noise * row_scale + row_shift).reshape(SHARDS * TOK_DEV, D).astype(jnp.bfloat16)


def setup_inputs(seed: int = 0) -> dict:
    sub_keys = jax.random.split(jax.random.key(seed), 17)
    w_up = jax.random.normal(sub_keys[6], (BLOCKS, D, FF), jnp.float32) / math.sqrt(D)
    w_down = jax.random.normal(sub_keys[7], (BLOCKS, FF, D), jnp.float32) / math.sqrt(FF)
    return {
        "tokens": shifted_rows(sub_keys[0], sub_keys[1], sub_keys[2]),
        "out_grad": shifted_rows(sub_keys[3], sub_keys[4], sub_keys[5]),
        "w_up": w_up.astype(jnp.bfloat16),
        "w_down": w_down.astype(jnp.bfloat16),
        "a_up_old": 0.3 * spd_draw(sub_keys[8], D, 0.5, 1.5),
        "s_up_old": 0.3 * spd_draw(sub_keys[9], FF, 0.5, 1.5),
        "a_down_old": 0.3 * spd_draw(sub_keys[10], FF, 0.5, 1.5),
        "s_down_old": 0.3 * spd_draw(sub_keys[11], D, 0.5, 1.5),
        "a_up_inv": spd_draw(sub_keys[12], D, 0.5, 1.5),
        "s_up_inv": spd_draw(sub_keys[13], FF, 0.5, 1.5),
        "a_down_inv": spd_draw(sub_keys[14], FF, 0.5, 1.5),
        "s_down_inv": spd_draw(sub_keys[15], D, 0.5, 1.5),
        "factor_decay": jax.random.uniform(sub_keys[16], (), jnp.float32, 0.6, 0.9),
    }


def cross_sum(left, right):
    return jnp.dot(left.T, right, preferred_element_type=jnp.float32)


def reference(tokens, out_grad, w_up, w_down, a_up_old, s_up_old, a_down_old, s_down_old,
              a_up_inv, s_up_inv, a_down_inv, s_down_inv, factor_decay):
    batch_total = SHARDS * TOK_DEV

    def shard_step(carry, rows_pair):
        tok_rows, grad_rows = rows_pair
        layer_ins = []
        pre_ups = []
        hiddens = []
        layer_in = tok_rows
        for block_idx in range(BLOCKS):
            pre_up = jnp.dot(layer_in, w_up[block_idx], preferred_element_type=jnp.float32).astype(jnp.bfloat16)
            hidden = gelu_fn(pre_up.astype(jnp.float32)).astype(jnp.bfloat16)
            layer_ins.append(layer_in)
            pre_ups.append(pre_up)
            hiddens.append(hidden)
            if block_idx + 1 < BLOCKS:
                layer_in = jnp.dot(hidden, w_down[block_idx], preferred_element_type=jnp.float32).astype(jnp.bfloat16)
        found = [[], [], [], [], [], []]
        grad_down = grad_rows
        for block_idx in reversed(range(BLOCKS)):
            hidden = hiddens[block_idx]
            layer_in = layer_ins[block_idx]
            d_hidden = jnp.dot(grad_down, w_down[block_idx].T, preferred_element_type=jnp.float32).astype(jnp.bfloat16)
            gelu_back = jax.vjp(gelu_fn, pre_ups[block_idx].astype(jnp.float32))[1]
            grad_up = gelu_back(d_hidden.astype(jnp.float32))[0].astype(jnp.bfloat16)
            terms = (cross_sum(layer_in, grad_up), cross_sum(hidden, grad_down),
                     cross_sum(layer_in, layer_in), cross_sum(grad_up, grad_up),
                     cross_sum(hidden, hidden), cross_sum(grad_down, grad_down))
            for slot, term in enumerate(terms):
                found[slot].insert(0, term)
            if block_idx > 0:
                grad_down = jnp.dot(grad_up, w_up[block_idx].T, preferred_element_type=jnp.float32).astype(jnp.bfloat16)
        return tuple(acc_sum + jnp.stack(items) for acc_sum, items in zip(carry, found)), None

    zero_init = (jnp.zeros((BLOCKS, D, FF), jnp.float32), jnp.zeros((BLOCKS, FF, D), jnp.float32),
                 jnp.zeros((BLOCKS, D, D), jnp.float32), jnp.zeros((BLOCKS, FF, FF), jnp.float32),
                 jnp.zeros((BLOCKS, FF, FF), jnp.float32), jnp.zeros((BLOCKS, D, D), jnp.float32))
    rows_in = (tokens.reshape(SHARDS, TOK_DEV, D), out_grad.reshape(SHARDS, TOK_DEV, D))
    totals = lax.scan(shard_step, zero_init, rows_in)[0]
    dw_up, dw_down, a_up, s_up, a_down, s_down = [total / batch_total for total in totals]
    decay_keep = factor_decay
    decay_fresh = 1.0 - factor_decay
    a_up_new = decay_keep * a_up_old + decay_fresh * a_up
    s_up_new = decay_keep * s_up_old + decay_fresh * s_up
    a_down_new = decay_keep * a_down_old + decay_fresh * a_down
    s_down_new = decay_keep * s_down_old + decay_fresh * s_down
    precond_up = jnp.einsum("bij,bjk->bik", jnp.einsum("bij,bjk->bik", a_up_inv, dw_up), s_up_inv)
    precond_down = jnp.einsum("bij,bjk->bik", jnp.einsum("bij,bjk->bik", a_down_inv, dw_down), s_down_inv)
    return (precond_up, precond_down, a_up_new, s_up_new, a_down_new, s_down_new)
```

```python
import functools
import jax
import jax.numpy as jnp
from jax import lax
from jax.experimental import pallas as pl
from jax.experimental.pallas import tpu as pltpu
from jax.sharding import PartitionSpec as P

C0 = 0.7978845608028654
C1 = C0 * 0.044715
BK = 256
ROWS = 1024
SUB = 64
BLOCKS = 60
PIECE = 1024
PIECES = BLOCKS * BK // PIECE
RING = 6
SLOT_ROWS = 992
VMEM_LIMIT = 67043328
PAIRS = [(i, j) for i in range(4) for j in range(i, 4)]
GRAM_H0, GRAM_U0, GRAM_Q1 = 0, 10, 11
GRAM_H1, DOWN1 = 12, 22
GRAM_G1, UP1, GRAM_U1, GRAM_E1 = 26, 36, 40, 41
UP0, DOWN0, GRAM_G0 = 42, 46, 50
STAGES = 8


def dot(left, right):
    return jnp.dot(left, right, preferred_element_type=jnp.float32)


def dot_nt(left, right):
    return lax.dot_general(left, right, (((1,), (1,)), ((), ())), preferred_element_type=jnp.float32)


def blk(index):
    return pl.ds(index * BK, BK)


class Exchange:
    def __init__(self, acc, slots, send, recv, free):
        self.acc, self.slots, self.send, self.recv, self.free = acc, slots, send, recv, free
        me = lax.axis_index("data")
        self.me = me
        self.core = lax.rem(me, 2)
        self.plane = (lax.rem(me // 2, 2), lax.rem(me // 4, 2))
        self.z = me // 8
        flip = lambda bit, step: me + (1 - 2 * bit) * step
        self.core_peer = flip(self.core, 1)
        self.plane_peer = (flip(self.plane[0], 2), flip(self.plane[1], 4))
        base = lax.rem(me, 8)
        self.z_peer = [base + 8 * lax.rem(self.z + d, 4) for d in (1, 2, 3)]

    def barrier(self):
        sem = pltpu.get_barrier_semaphore()
        peers = [self.core_peer, *self.plane_peer, *self.z_peer]
        for peer in peers:
            pl.semaphore_signal(sem, inc=1, device_id=(peer,), device_id_type=pl.DeviceIdType.MESH)
        pl.semaphore_wait(sem, len(peers))

    def rows(self, start, size):
        return self.acc.at[pl.ds(pl.multiple_of(start, 16), size), :]

    def spots(self, piece, color):
        first, second = (0, 1) if color == 0 else (1, 0)
        base1 = piece * PIECE + self.core * 512 + color * 256
        bit1, bit2 = self.plane[first], self.plane[second]
        base2 = base1 + bit1 * 128
        base3 = base2 + bit2 * 64
        return first, second, bit1, bit2, base1, base2, base3

    def copies(self, piece, stage):
        ring = piece % RING
        slot = self.slots.at[ring]
        found = []

        def add(number, src, dst, peer, keep=None, got=None):
            sem = stage * 6 + number
            found.append((pltpu.make_async_remote_copy(
                src_ref=src, dst_ref=dst, send_sem=self.send.at[ring, sem], recv_sem=self.recv.at[ring, sem],
                device_id=(peer,), device_id_type=pl.DeviceIdType.MESH), keep, got, peer))

        top = piece * PIECE
        if stage == 0:
            got = slot.at[pl.ds(0, 512), :]
            add(0, self.rows(top + (1 - self.core) * 512, 512), got, self.core_peer,
                (top + self.core * 512, 512), got)
        elif stage == 7:
            mine = self.rows(top + self.core * 512, 512)
            add(0, mine, mine, self.core_peer)
        for color in range(2):
            first, second, bit1, bit2, base1, base2, base3 = self.spots(piece, color)
            if stage == 1:
                got = slot.at[pl.ds(512 + color * 128, 128), :]
                add(color, self.rows(base1 + (1 - bit1) * 128, 128), got, self.plane_peer[first], (base2, 128), got)
            elif stage == 2:
                got = slot.at[pl.ds(768 + color * 64, 64), :]
                add(color, self.rows(base2 + (1 - bit2) * 64, 64), got, self.plane_peer[second], (base3, 64), got)
            elif stage == 3:
                for d in range(3):
                    got = slot.at[pl.ds(896 + color * 48 + d * 16, 16), :]
                    peer_z = lax.rem(self.z + d + 1, 4)
                    add(color * 3 + d, self.rows(base3 + peer_z * 16, 16), got, self.z_peer[d],
                        (base3 + self.z * 16, 16), got)
            elif stage == 4:
                mine = self.rows(base3 + self.z * 16, 16)
                for d in range(3):
                    add(color * 3 + d, mine, mine, self.z_peer[d])
            elif stage == 5:
                mine = self.rows(base3, 64)
                add(color, mine, mine, self.plane_peer[second])
            elif stage == 6:
                mine = self.rows(base2, 128)
                add(color, mine, mine, self.plane_peer[first])
        return found

    def credits(self, piece, stage):
        colors = 1 if stage == 0 else 2
        return [self.free.at[piece % RING, 2 * stage + color] for color in range(colors)]

    def start(self, piece, stage):
        found = self.copies(piece, stage)
        if stage >= STAGES // 2:
            credits = self.credits(piece, STAGES - 1 - stage)
            for credit in credits:
                pl.semaphore_wait(credit, len(found) // len(credits))
        for copy, *_ in found:
            copy.start()

    def finish(self, piece, stage):
        found = self.copies(piece, stage)
        for copy, *_ in found:
            copy.wait()
        if stage < STAGES // 2:
            credits = self.credits(piece, stage)
            per = len(found) // len(credits)
            for number, (_, _, _, peer) in enumerate(found):
                pl.semaphore_signal(credits[number // per], inc=1, device_id=(peer,),
                                    device_id_type=pl.DeviceIdType.MESH)
            for _, keep, got, _ in found:
                self.rows(*keep)[...] += got[...]

    def slot_of_time(self, events):
        for piece, stage in events:
            if stage > 0:
                self.finish(piece, stage - 1)
        for piece, stage in events:
            if stage < STAGES:
                self.start(piece, stage)


def cdf_of(pre):
    square = pre * pre
    return square, 0.5 * jnp.tanh(pre * (C1 * square + C0)) + 0.5


def slope_of(pre, square, cdf):
    return cdf * (((1.0 - cdf) * pre) * (6.0 * C1 * square + 2.0 * C0) + 1.0)


def produce_forward(col, u, w_ref, z_ref, h_ref):
    z_ref[...] = dot(u[...], w_ref[:, blk(col)]).astype(jnp.bfloat16)
    for row in range(0, ROWS, SUB):
        pre = z_ref[row:row + SUB, :].astype(jnp.float32)
        _, cdf = cdf_of(pre)
        h_ref[row:row + SUB, blk(col)] = (pre * cdf).astype(jnp.bfloat16)


def produce_both(col, u, w_ref, q, wd_ref, z_ref, d_ref, h_ref, g, off):
    z_ref[...] = dot(u[...], w_ref[:, blk(col)]).astype(jnp.bfloat16)
    d_ref[...] = dot_nt(q[...], wd_ref[blk(col), :]).astype(jnp.bfloat16)
    for row in range(0, ROWS, SUB):
        pre = z_ref[row:row + SUB, :].astype(jnp.float32)
        d_hidden = d_ref[row:row + SUB, :].astype(jnp.float32)
        square, cdf = cdf_of(pre)
        h_ref[row:row + SUB, blk(col)] = (pre * cdf).astype(jnp.bfloat16)
        g[pl.ds(off + row, SUB), blk(col)] = (d_hidden * slope_of(pre, square, cdf)).astype(jnp.bfloat16)


def kernel(tok_hbm, grad_hbm, w_up_hbm, w_down_hbm, out_hbm,
           acc, slots, tok, grad, mid, g1, w_up, w_down, z0, z1, d0, d1, h_ref, t_ref, ht_ref, small,
           send, recv, free, tok_sem, grad_sem, w_sem, out_sem):
    tiles = tok.shape[0] // ROWS
    w_copies = [pltpu.make_async_copy(w_up_hbm, w_up, w_sem.at[0]),
                pltpu.make_async_copy(w_down_hbm, w_down, w_sem.at[1])]

    def tile_copies(i):
        rows = pl.ds(pl.multiple_of(i * ROWS, ROWS), ROWS)
        return (pltpu.make_async_copy(tok_hbm.at[rows, :], tok.at[rows, :], tok_sem.at[i]),
                pltpu.make_async_copy(grad_hbm.at[rows, :], grad.at[rows, :], grad_sem.at[i]))

    for copy in w_copies:
        copy.start()
    for i in range(tiles):
        for copy in tile_copies(i):
            copy.start()
    exchange = Exchange(acc, slots, send, recv, free)
    exchange.barrier()

    @pl.loop(0, BLOCKS)
    def _(n):
        acc[pl.ds(pl.multiple_of(n * BK, BK), BK), :] = jnp.zeros((BK, BK), jnp.float32)

    for copy in w_copies:
        copy.wait()
    zs, ds_ = (z0, z1), (d0, d1)

    def out_copy(piece):
        rows = pl.ds(piece * PIECE, PIECE)
        return pltpu.make_async_copy(acc.at[rows, :], out_hbm.at[rows, :], out_sem.at[piece])

    starts = {}

    def events_at(now):
        return [(piece, now - first) for piece, first in starts.items() if 0 <= now - first <= STAGES]

    def fire(events):
        if events:
            exchange.slot_of_time(events)
            for piece, stage in events:
                if stage == STAGES:
                    out_copy(piece).start()

    def hooks(i, first):
        for n in range(tiles):
            events = events_at(first + n)
            if events:
                pl.when(i == n)(functools.partial(fire, events))

    def add_to(slot, value):
        acc[blk(slot), :] += value

    def gram_column(first, col, x):
        for i in range(col + 1):
            add_to(first + PAIRS.index((i, col)), dot(t_ref[blk(i), :], x(col)))

    def views(i):
        off = pl.multiple_of(i * ROWS, ROWS)
        rows = pl.ds(off, ROWS)
        return off, tok.at[rows, :], grad.at[rows, :], mid.at[rows, :]

    @pl.loop(0, tiles)
    def _(i):
        off, u, q, nxt = views(i)
        for copy in tile_copies(i):
            copy.wait()
        hx = lambda col: h_ref[:, blk(col)]

        def produce(col):
            produce_forward(col, u, w_up.at[0], zs[col % 2], h_ref)
            t_ref[blk(col), :] = h_ref[:, blk(col)].T

        produce(0)
        small[...] = u[...].T
        add_to(GRAM_U0, dot(small[...], u[...]))
        produce(1)
        gram_column(GRAM_H0, 0, hx)
        small[...] = q[...].T
        add_to(GRAM_Q1, dot(small[...], q[...]))
        produce(2)
        gram_column(GRAM_H0, 1, hx)
        produce(3)
        gram_column(GRAM_H0, 2, hx)
        nxt[...] = dot(h_ref[...], w_down[0]).astype(jnp.bfloat16)
        gram_column(GRAM_H0, 3, hx)

    starts.update({0: 8, 1: 9, 2: 10})

    @pl.loop(0, tiles)
    def _(i):
        hooks(i, 8)
        off, _, q, u = views(i)
        hx = lambda col: h_ref[:, blk(col)]

        def produce(col):
            produce_both(col, u, w_up.at[1], q, w_down.at[1], zs[col % 2], ds_[col % 2], h_ref, g1, off)
            t_ref[blk(col), :] = h_ref[:, blk(col)].T

        def consume(col):
            gram_column(GRAM_H1, col, hx)
            add_to(DOWN1 + col, dot(t_ref[blk(col), :], q[...]))

        produce(0)
        for col in range(1, 4):
            produce(col)
            consume(col - 1)
        consume(3)

    starts.update({3: 16, 4: 17, 5: 18})

    @pl.loop(0, tiles)
    def _(i):
        hooks(i, 16)
        off, _, _, u = views(i)
        rows = pl.ds(off, ROWS)
        gx = lambda col: g1[rows, blk(col)]
        small[...] = u[...].T
        add_to(GRAM_U1, dot(small[...], u[...]))
        for col in range(4):
            t_ref[blk(col), :] = gx(col).T
            add_to(UP1 + col, dot(small[...], gx(col)))
            gram_column(GRAM_G1, col, gx)
        u[...] = dot_nt(g1[rows, :], w_up[1]).astype(jnp.bfloat16)
        small[...] = u[...].T
        add_to(GRAM_E1, dot(small[...], u[...]))

    starts.update({6: 24, 7: 25, 8: 26, 9: 27})

    @pl.loop(0, tiles)
    def _(i):
        hooks(i, 24)
        off, u, _, q = views(i)
        rows = pl.ds(off, ROWS)

        def produce(col):
            produce_both(col, u, w_up.at[0], q, w_down.at[0], zs[col % 2], ds_[col % 2], h_ref, g1, off)
            ht_ref[blk(col % 2), :] = h_ref[:, blk(col)].T

        def consume(col):
            add_to(UP0 + col, dot(small[...], g1[rows, blk(col)]))
            add_to(DOWN0 + col, dot(ht_ref[blk(col % 2), :], q[...]))

        small[...] = u[...].T
        produce(0)
        for col in range(1, 4):
            produce(col)
            consume(col - 1)
        consume(3)

    starts.update({10: 32, 11: 33})

    def gram_row(row, now):
        halves = 2 if row < 2 else 1
        per = tiles // halves
        for half in range(halves):
            fire(events_at(now + half))

            @pl.loop(half * per, (half + 1) * per)
            def _(i):
                rows = pl.ds(pl.multiple_of(i * ROWS, ROWS), ROWS)
                small[...] = g1[rows, blk(row)].T
                for col in range(row, 4):
                    add_to(GRAM_G0 + PAIRS.index((row, col)), dot(small[...], g1[rows, blk(col)]))
        return now + halves

    now = gram_row(0, 32)
    starts[12] = max(now, 34)
    now = gram_row(1, now)
    starts[13] = now
    now = gram_row(2, now)
    now = gram_row(3, now)
    starts[14] = now
    while now <= max(starts.values()) + STAGES:
        fire(events_at(now))
        now += 1
    for piece in range(PIECES):
        out_copy(piece).wait()


def statistics(tok, grad, w_up, w_down):
    rows = tok.shape[0]
    tiles = rows // ROWS
    bf = lambda *shape: pltpu.VMEM(shape, jnp.bfloat16)
    any_spec = pl.BlockSpec(memory_space=pl.ANY)
    dma = pltpu.SemaphoreType.DMA
    return pl.pallas_call(
        kernel, name="statistics", in_specs=[any_spec] * 4, out_specs=any_spec,
        out_shape=jax.ShapeDtypeStruct((BLOCKS * BK, BK), jnp.float32),
        scratch_shapes=[
            pltpu.VMEM((BLOCKS * BK, BK), jnp.float32), pltpu.VMEM((RING, SLOT_ROWS, BK), jnp.float32),
            bf(rows, BK), bf(rows, BK), bf(rows, BK), bf(rows, 4 * BK), bf(*w_up.shape), bf(*w_down.shape),
            bf(ROWS, BK), bf(ROWS, BK), bf(ROWS, BK), bf(ROWS, BK),
            bf(ROWS, 4 * BK), bf(4 * BK, ROWS), bf(2 * BK, ROWS), bf(BK, ROWS),
            dma((RING, 6 * STAGES)), dma((RING, 6 * STAGES)),
            pltpu.SemaphoreType.REGULAR((RING, STAGES)), dma((tiles,)), dma((tiles,)), dma((2,)), dma((PIECES,))],
        cost_estimate=pl.CostEstimate(flops=100 * 10 ** 9, bytes_accessed=30 << 20, transcendentals=0),
        compiler_params=pltpu.CompilerParams(vmem_limit_bytes=VMEM_LIMIT, collective_id=0, has_side_effects=True),
    )(tok, grad, w_up, w_down)


def full_gram(packed, first):
    take = lambda n: packed[(first + n) * BK:(first + n + 1) * BK]
    pick = lambda i, j: take(PAIRS.index((i, j))) if i <= j else take(PAIRS.index((j, i))).T
    return jnp.concatenate([jnp.concatenate([pick(i, j) for j in range(4)], axis=1) for i in range(4)], axis=0)


def solution(mesh):
    axis_size = mesh.shape["data"]
    high = lax.Precision.HIGHEST

    def precise(left, right):
        return jnp.dot(left, right, precision=high, preferred_element_type=jnp.float32)

    def local_step(tok, grad, w_up, w_down, a_up_old, s_up_old, a_down_old, s_down_old,
                   a_up_inv, s_up_inv, a_down_inv, s_down_inv, factor_decay):
        packed = statistics(tok, grad, w_up, w_down)
        scale = 1.0 / (tok.shape[0] * axis_size)
        block = lambda n: packed[n * BK:(n + 1) * BK]
        across = lambda n: jnp.concatenate([block(n + i) for i in range(4)], axis=1)
        down = lambda n: packed[n * BK:(n + 4) * BK]
        keep, fresh = factor_decay, (1.0 - factor_decay) * scale
        stack = lambda first, second: jnp.stack([first, second])
        chain = lambda left, mid, right: precise(precise(left, mid * scale), right)
        return (stack(chain(a_up_inv[0], across(UP0), s_up_inv[0]), chain(a_up_inv[1], across(UP1), s_up_inv[1])),
                stack(chain(a_down_inv[0], down(DOWN0), s_down_inv[0]), chain(a_down_inv[1], down(DOWN1), s_down_inv[1])),
                keep * a_up_old + fresh * stack(block(GRAM_U0), block(GRAM_U1)),
                keep * s_up_old + fresh * stack(full_gram(packed, GRAM_G0), full_gram(packed, GRAM_G1)),
                keep * a_down_old + fresh * stack(full_gram(packed, GRAM_H0), full_gram(packed, GRAM_H1)),
                keep * s_down_old + fresh * stack(block(GRAM_E1), block(GRAM_Q1)))

    batch_spec = P("data", None)
    replicated = P()
    return jax.shard_map(local_step, mesh=mesh, in_specs=(batch_spec, batch_spec) + (replicated,) * 11,
                         out_specs=(replicated,) * 6, check_vma=False)
```

```python
import functools
import jax
import jax.numpy as jnp
from jax import lax
from jax.experimental import pallas as pl
from jax.experimental.pallas import tpu as pltpu
from jax.sharding import PartitionSpec as P

C0 = 0.7978845608028654
C1 = C0 * 0.044715
BK = 256
ROWS = 1024
SUB = 64
BLOCKS = 60
PIECE = 1024
PIECES = BLOCKS * BK // PIECE
RING = 8
CORE_RING = 3
SLOT_ROWS = 480
VMEM_LIMIT = 67043328
PAIRS = [(i, j) for i in range(4) for j in range(i, 4)]
GRAM_H0, GRAM_U0, GRAM_Q1 = 0, 10, 11
GRAM_H1, DOWN1 = 12, 22
GRAM_G1, UP1, GRAM_U1, GRAM_E1 = 26, 36, 40, 41
UP0, DOWN0, GRAM_G0 = 42, 46, 50
STAGES = 8
FIRST = (8, 9, 10, 16, 17, 18, 24, 25, 26, 28, 32, 33, 35, 36, 38)
SLOW_UNTIL = 36


def times_of(first):
    times = [first]
    for _ in range(STAGES):
        times.append(times[-1] + (2 if times[-1] < SLOW_UNTIL else 1))
    return times


TIMES = [times_of(first) for first in FIRST]


def dot(left, right):
    return jnp.dot(left, right, preferred_element_type=jnp.float32)


def dot_nt(left, right):
    return lax.dot_general(left, right, (((1,), (1,)), ((), ())), preferred_element_type=jnp.float32)


def blk(index):
    return pl.ds(index * BK, BK)


class Exchange:
    def __init__(self, acc, core_slots, slots, send, recv, free):
        self.core_slots = core_slots
        self.acc, self.slots, self.send, self.recv, self.free = acc, slots, send, recv, free
        me = lax.axis_index("data")
        self.me = me
        self.core = lax.rem(me, 2)
        self.plane = (lax.rem(me // 2, 2), lax.rem(me // 4, 2))
        self.z = me // 8
        flip = lambda bit, step: me + (1 - 2 * bit) * step
        self.core_peer = flip(self.core, 1)
        self.plane_peer = (flip(self.plane[0], 2), flip(self.plane[1], 4))
        base = lax.rem(me, 8)
        self.z_peer = [base + 8 * lax.rem(self.z + d, 4) for d in (1, 2, 3)]

    def barrier(self):
        sem = pltpu.get_barrier_semaphore()
        peers = [self.core_peer, *self.plane_peer, *self.z_peer]
        for peer in peers:
            pl.semaphore_signal(sem, inc=1, device_id=(peer,), device_id_type=pl.DeviceIdType.MESH)
        pl.semaphore_wait(sem, len(peers))

    def rows(self, start, size):
        return self.acc.at[pl.ds(pl.multiple_of(start, 16), size), :]

    def spots(self, piece, color):
        first, second = (0, 1) if color == 0 else (1, 0)
        base1 = piece * PIECE + self.core * 512 + color * 256
        bit1, bit2 = self.plane[first], self.plane[second]
        base2 = base1 + bit1 * 128
        base3 = base2 + bit2 * 64
        return first, second, bit1, bit2, base1, base2, base3

    def copies(self, piece, stage):
        ring = piece % RING
        slot = self.slots.at[ring]
        found = []

        def add(number, src, dst, peer, keep=None, got=None):
            sem = stage * 6 + number
            found.append((pltpu.make_async_remote_copy(
                src_ref=src, dst_ref=dst, send_sem=self.send.at[ring, sem], recv_sem=self.recv.at[ring, sem],
                device_id=(peer,), device_id_type=pl.DeviceIdType.MESH), keep, got, peer))

        top = piece * PIECE
        if stage == 0:
            got = self.core_slots.at[piece % CORE_RING]
            add(0, self.rows(top + (1 - self.core) * 512, 512), got, self.core_peer,
                (top + self.core * 512, 512), got)
        elif stage == 7:
            mine = self.rows(top + self.core * 512, 512)
            add(0, mine, mine, self.core_peer)
        for color in range(2):
            first, second, bit1, bit2, base1, base2, base3 = self.spots(piece, color)
            if stage == 1:
                got = slot.at[pl.ds(color * 128, 128), :]
                add(color, self.rows(base1 + (1 - bit1) * 128, 128), got, self.plane_peer[first], (base2, 128), got)
            elif stage == 2:
                got = slot.at[pl.ds(256 + color * 64, 64), :]
                add(color, self.rows(base2 + (1 - bit2) * 64, 64), got, self.plane_peer[second], (base3, 64), got)
            elif stage == 3:
                for d in range(3):
                    got = slot.at[pl.ds(384 + color * 48 + d * 16, 16), :]
                    peer_z = lax.rem(self.z + d + 1, 4)
                    add(color * 3 + d, self.rows(base3 + peer_z * 16, 16), got, self.z_peer[d],
                        (base3 + self.z * 16, 16), got)
            elif stage == 4:
                mine = self.rows(base3 + self.z * 16, 16)
                for d in range(3):
                    add(color * 3 + d, mine, mine, self.z_peer[d])
            elif stage == 5:
                mine = self.rows(base3, 64)
                add(color, mine, mine, self.plane_peer[second])
            elif stage == 6:
                mine = self.rows(base2, 128)
                add(color, mine, mine, self.plane_peer[first])
        return found

    def credits(self, piece, stage):
        colors = 1 if stage == 0 else 2
        return [self.free.at[piece % RING, 2 * stage + color] for color in range(colors)]

    def start(self, piece, stage):
        found = self.copies(piece, stage)
        back = 0 if stage == 2 else STAGES - 1 - stage
        if stage == 2 or STAGES // 2 <= stage < STAGES - 1:
            credits = self.credits(piece, back)
            peers = 1 if back == 0 else len(found) // len(credits)
            for credit in credits:
                pl.semaphore_wait(credit, peers)
        for copy, *_ in found:
            copy.start()

    def finish(self, piece, stage):
        found = self.copies(piece, stage)
        for copy, *_ in found:
            copy.wait()
        if stage < STAGES // 2:
            for _, keep, got, _ in found:
                self.rows(*keep)[...] += got[...]
            credits = self.credits(piece, stage)
            per = len(found) // len(credits)
            for number, (_, _, _, peer) in enumerate(found):
                pl.semaphore_signal(credits[number // per], inc=1, device_id=(peer,),
                                    device_id_type=pl.DeviceIdType.MESH)

    def slot_of_time(self, events):
        for piece, stage in events:
            if stage > 0:
                self.finish(piece, stage - 1)
            if stage < STAGES:
                self.start(piece, stage)


def cdf_of(pre):
    square = pre * pre
    return square, 0.5 * jnp.tanh(pre * (C1 * square + C0)) + 0.5


def slope_of(pre, square, cdf):
    return cdf * (((1.0 - cdf) * pre) * (6.0 * C1 * square + 2.0 * C0) + 1.0)


def produce_forward(col, u, w_ref, z_ref, h_ref):
    z_ref[...] = dot(u[...], w_ref[:, blk(col)]).astype(jnp.bfloat16)
    for row in range(0, ROWS, SUB):
        pre = z_ref[row:row + SUB, :].astype(jnp.float32)
        _, cdf = cdf_of(pre)
        h_ref[row:row + SUB, blk(col)] = (pre * cdf).astype(jnp.bfloat16)


def produce_both(col, u, w_ref, q, wd_ref, z_ref, d_ref, h_ref, g, off):
    z_ref[...] = dot(u[...], w_ref[:, blk(col)]).astype(jnp.bfloat16)
    d_ref[...] = dot_nt(q[...], wd_ref[blk(col), :]).astype(jnp.bfloat16)
    for row in range(0, ROWS, SUB):
        pre = z_ref[row:row + SUB, :].astype(jnp.float32)
        d_hidden = d_ref[row:row + SUB, :].astype(jnp.float32)
        square, cdf = cdf_of(pre)
        h_ref[row:row + SUB, blk(col)] = (pre * cdf).astype(jnp.bfloat16)
        g[pl.ds(off + row, SUB), blk(col)] = (d_hidden * slope_of(pre, square, cdf)).astype(jnp.bfloat16)


def kernel(tok_hbm, grad_hbm, w_up_hbm, w_down_hbm, out_hbm,
           acc, core_slots, slots, tok, grad, mid, g1, w_up, w_down, z0, z1, d0, d1, h_ref, t_ref,
           send, recv, free, tok_sem, grad_sem, w_sem, out_sem):
    tiles = tok.shape[0] // ROWS
    w_copies = [pltpu.make_async_copy(w_up_hbm, w_up, w_sem.at[0]),
                pltpu.make_async_copy(w_down_hbm, w_down, w_sem.at[1])]

    def tile_copies(i):
        rows = pl.ds(pl.multiple_of(i * ROWS, ROWS), ROWS)
        return (pltpu.make_async_copy(tok_hbm.at[rows, :], tok.at[rows, :], tok_sem.at[i]),
                pltpu.make_async_copy(grad_hbm.at[rows, :], grad.at[rows, :], grad_sem.at[i]))

    for copy in w_copies:
        copy.start()
    for i in range(tiles):
        for copy in tile_copies(i):
            copy.start()
    exchange = Exchange(acc, core_slots, slots, send, recv, free)
    exchange.barrier()

    @pl.loop(0, BLOCKS)
    def _(n):
        acc[pl.ds(pl.multiple_of(n * BK, BK), BK), :] = jnp.zeros((BK, BK), jnp.float32)

    for copy in w_copies:
        copy.wait()
    zs, ds_ = (z0, z1), (d0, d1)

    def out_copy(piece):
        rows = pl.ds(piece * PIECE, PIECE)
        return pltpu.make_async_copy(acc.at[rows, :], out_hbm.at[rows, :], out_sem.at[piece])

    def events_at(now):
        return [(piece, stage) for piece in range(PIECES) for stage in range(STAGES + 1) if TIMES[piece][stage] == now]

    def fire(events):
        if events:
            exchange.slot_of_time(events)
            for piece, stage in events:
                if stage == STAGES:
                    out_copy(piece).start()

    def hooks(i, first):
        for n in range(tiles):
            events = events_at(first + n)
            if events:
                pl.when(i == n)(functools.partial(fire, events))

    def add_to(slot, value):
        acc[blk(slot), :] += value

    def gram_column(first, col, x):
        for i in range(col + 1):
            add_to(first + PAIRS.index((i, col)), dot(t_ref[blk(i), :], x(col)))

    def views(i):
        off = pl.multiple_of(i * ROWS, ROWS)
        rows = pl.ds(off, ROWS)
        return off, tok.at[rows, :], grad.at[rows, :], mid.at[rows, :]

    @pl.loop(0, tiles)
    def _(i):
        off, u, q, nxt = views(i)
        for copy in tile_copies(i):
            copy.wait()
        hx = lambda col: h_ref[:, blk(col)]

        def produce(col):
            produce_forward(col, u, w_up.at[0], zs[col % 2], h_ref)
            t_ref[blk(col), :] = h_ref[:, blk(col)].T

        small = t_ref.at[blk(3), :]
        produce(0)
        small[...] = u[...].T
        add_to(GRAM_U0, dot(small[...], u[...]))
        produce(1)
        gram_column(GRAM_H0, 0, hx)
        small[...] = q[...].T
        add_to(GRAM_Q1, dot(small[...], q[...]))
        produce(2)
        gram_column(GRAM_H0, 1, hx)
        produce(3)
        gram_column(GRAM_H0, 2, hx)
        nxt[...] = dot(h_ref[...], w_down[0]).astype(jnp.bfloat16)
        gram_column(GRAM_H0, 3, hx)

    @pl.loop(0, tiles)
    def _(i):
        hooks(i, 8)
        off, _, q, u = views(i)
        hx = lambda col: h_ref[:, blk(col)]

        def produce(col):
            produce_both(col, u, w_up.at[1], q, w_down.at[1], zs[col % 2], ds_[col % 2], h_ref, g1, off)
            t_ref[blk(col), :] = h_ref[:, blk(col)].T

        def consume(col):
            gram_column(GRAM_H1, col, hx)
            add_to(DOWN1 + col, dot(t_ref[blk(col), :], q[...]))

        produce(0)
        for col in range(1, 4):
            produce(col)
            consume(col - 1)
        consume(3)

    @pl.loop(0, tiles)
    def _(i):
        hooks(i, 16)
        off, _, _, u = views(i)
        rows = pl.ds(off, ROWS)
        gx = lambda col: g1[rows, blk(col)]
        small = h_ref.at[blk(0), :]
        small[...] = u[...].T
        add_to(GRAM_U1, dot(small[...], u[...]))
        for col in range(4):
            t_ref[blk(col), :] = gx(col).T
            add_to(UP1 + col, dot(small[...], gx(col)))
            gram_column(GRAM_G1, col, gx)
        u[...] = dot_nt(g1[rows, :], w_up[1]).astype(jnp.bfloat16)
        small[...] = u[...].T
        add_to(GRAM_E1, dot(small[...], u[...]))

    @pl.loop(0, tiles)
    def _(i):
        hooks(i, 24)
        off, u, _, q = views(i)
        rows = pl.ds(off, ROWS)

        def produce(col):
            produce_both(col, u, w_up.at[0], q, w_down.at[0], zs[col % 2], ds_[col % 2], h_ref, g1, off)
            t_ref[blk(col % 3), :] = h_ref[:, blk(col)].T

        def consume(col):
            add_to(UP0 + col, dot(small[...], g1[rows, blk(col)]))
            add_to(DOWN0 + col, dot(t_ref[blk(col % 3), :], q[...]))

        small = t_ref.at[blk(3), :]
        small[...] = u[...].T
        produce(0)
        for col in range(1, 4):
            produce(col)
            consume(col - 1)
        consume(3)

    def gram_row(row, now):
        halves = 2 if row < 2 else 1
        per = tiles // halves
        for half in range(halves):
            fire(events_at(now + half))

            @pl.loop(half * per, (half + 1) * per)
            def _(i):
                rows = pl.ds(pl.multiple_of(i * ROWS, ROWS), ROWS)
                small = t_ref.at[blk(0), :]
                small[...] = g1[rows, blk(row)].T
                for col in range(row, 4):
                    add_to(GRAM_G0 + PAIRS.index((row, col)), dot(small[...], g1[rows, blk(col)]))
        return now + halves

    now = 32
    for row in range(4):
        now = gram_row(row, now)
    while now <= TIMES[-1][-1]:
        fire(events_at(now))
        now += 1
    for piece in range(PIECES):
        out_copy(piece).wait()


def statistics(tok, grad, w_up, w_down):
    rows = tok.shape[0]
    tiles = rows // ROWS
    bf = lambda *shape: pltpu.VMEM(shape, jnp.bfloat16)
    any_spec = pl.BlockSpec(memory_space=pl.ANY)
    dma = pltpu.SemaphoreType.DMA
    return pl.pallas_call(
        kernel, name="statistics", in_specs=[any_spec] * 4, out_specs=any_spec,
        out_shape=jax.ShapeDtypeStruct((BLOCKS * BK, BK), jnp.float32),
        scratch_shapes=[
            pltpu.VMEM((BLOCKS * BK, BK), jnp.float32), pltpu.VMEM((CORE_RING, 512, BK), jnp.float32),
            pltpu.VMEM((RING, SLOT_ROWS, BK), jnp.float32),
            bf(rows, BK), bf(rows, BK), bf(rows, BK), bf(rows, 4 * BK), bf(*w_up.shape), bf(*w_down.shape),
            bf(ROWS, BK), bf(ROWS, BK), bf(ROWS, BK), bf(ROWS, BK),
            bf(ROWS, 4 * BK), bf(4 * BK, ROWS),
            dma((RING, 6 * STAGES)), dma((RING, 6 * STAGES)),
            pltpu.SemaphoreType.REGULAR((RING, STAGES)), dma((tiles,)), dma((tiles,)), dma((2,)), dma((PIECES,))],
        cost_estimate=pl.CostEstimate(flops=100 * 10 ** 9, bytes_accessed=30 << 20, transcendentals=0),
        compiler_params=pltpu.CompilerParams(vmem_limit_bytes=VMEM_LIMIT, collective_id=0, has_side_effects=True),
    )(tok, grad, w_up, w_down)


def precise(left, right):
    return jnp.dot(left, right, precision=lax.Precision.HIGHEST, preferred_element_type=jnp.float32)


WIDTH = 4 * BK
STEPS = 16
DEPTH = 4


def finish_kernel(scale, decay, packed_hbm, a_up_old, s_up_old, a_down_old, s_down_old,
                  a_up_inv, s_up_inv, a_down_inv, s_down_inv,
                  p_up, p_down, a_up_new, s_up_new, a_down_new, s_down_new,
                  packed, wide_up, wide_down, small_up, small_down, old_ring, new_ring,
                  old_a, old_s, new_a, new_s, mid_up, mid_down, done_up, done_down,
                  pk_sem, inv_sem, old_sem, new_sem, small_sem, done_sem):
    keep = decay[0]
    fresh = (1.0 - decay[0]) * scale

    def pk_copy(piece):
        rows = pl.ds(piece * PIECE, PIECE)
        return pltpu.make_async_copy(packed_hbm.at[rows, :], packed.at[rows, :], pk_sem.at[piece])

    inv_copies = [pltpu.make_async_copy(a_up_inv, small_up, inv_sem.at[0]),
                  pltpu.make_async_copy(s_down_inv, small_down, inv_sem.at[1])]
    for b in range(2):
        inv_copies.append(pltpu.make_async_copy(s_up_inv.at[b], wide_up.at[b], inv_sem.at[2 + 2 * b]))
        inv_copies.append(pltpu.make_async_copy(a_down_inv.at[b], wide_down.at[b], inv_sem.at[3 + 2 * b]))
    grams = [(a_down_old, a_down_new, 0, GRAM_H0), (a_down_old, a_down_new, 1, GRAM_H1),
             (s_up_old, s_up_new, 1, GRAM_G1), (s_up_old, s_up_new, 0, GRAM_G0)]

    def old_copy(step):
        old, _, b, _ = grams[step // 4]
        return pltpu.make_async_copy(old.at[b, pl.ds(step % 4 * BK, BK), :], old_ring.at[step % DEPTH],
                                     old_sem.at[step % DEPTH])

    def new_copy(step):
        _, new, b, _ = grams[step // 4]
        return pltpu.make_async_copy(new_ring.at[step % DEPTH], new.at[b, pl.ds(step % 4 * BK, BK), :],
                                     new_sem.at[step % DEPTH])

    small_ins = [pltpu.make_async_copy(a_up_old, old_a, small_sem.at[0]),
                 pltpu.make_async_copy(s_down_old, old_s, small_sem.at[1])]
    small_outs = [pltpu.make_async_copy(new_a, a_up_new, small_sem.at[2]),
                  pltpu.make_async_copy(new_s, s_down_new, small_sem.at[3])]
    waited = set()

    def block(n):
        piece = n * BK // PIECE
        if piece not in waited:
            waited.add(piece)
            pk_copy(piece).wait()
        return packed[blk(n), :]

    def update(step):
        _, _, _, first = grams[step // 4]
        row = step % 4
        old_copy(step).wait()
        if step >= DEPTH:
            new_copy(step - DEPTH).wait()
        for col in range(4):
            pair = (min(row, col), max(row, col))
            value = block(first + PAIRS.index(pair))
            value = value if row <= col else value.T
            new_ring[step % DEPTH, :, blk(col)] = keep * old_ring[step % DEPTH, :, blk(col)] + fresh * value
        new_copy(step).start()
        if step + DEPTH < STEPS:
            old_copy(step + DEPTH).start()

    for step in range(DEPTH):
        old_copy(step).start()
    for piece in range(PIECES):
        pk_copy(piece).start()
    for copy in small_ins + inv_copies:
        copy.start()

    def chain_up(b, first):
        if b == 1:
            inv_copies[0].wait()
        for col in range(4):
            mid_up[:, blk(col)] = precise(small_up[b], block(first + col) * scale)

    def chain_up_end(b, col):
        if col == 0:
            inv_copies[2 + 2 * b].wait()
        done_up[b, :, blk(col)] = precise(mid_up[...], wide_up[b, :, blk(col)])
        if col == 3:
            pltpu.make_async_copy(done_up.at[b], p_up.at[b], done_sem.at[2 * b]).start()

    def chain_down(b, first, row):
        if row == 0:
            inv_copies[3 + 2 * b].wait()
            if b == 1:
                inv_copies[1].wait()
            for n in range(4):
                block(first + n)
        mid_down[...] = precise(wide_down[b, blk(row), :], packed[first * BK:(first + 4) * BK, :] * scale)
        done_down[b, blk(row), :] = precise(mid_down[...], small_down[b])
        if row == 3:
            pltpu.make_async_copy(done_down.at[b], p_down.at[b], done_sem.at[2 * b + 1]).start()

    for step in range(4):
        update(step)
    for n in range(4):
        chain_down(1, DOWN1, n)
        update(4 + n)
    chain_up(1, UP1)
    for n in range(4):
        chain_up_end(1, n)
        update(8 + n)
    for n in range(4):
        chain_down(0, DOWN0, n)
        update(12 + n)
    for copy in small_ins:
        copy.wait()
    for b, first in ((0, GRAM_U0), (1, GRAM_U1)):
        new_a[b] = keep * old_a[b] + fresh * block(first)
    for b, first in ((0, GRAM_E1), (1, GRAM_Q1)):
        new_s[b] = keep * old_s[b] + fresh * block(first)
    for copy in small_outs:
        copy.start()
    chain_up(0, UP0)
    for n in range(4):
        chain_up_end(0, n)
    for step in range(STEPS - DEPTH, STEPS):
        new_copy(step).wait()
    for copy in small_outs:
        copy.wait()
    for b in range(2):
        pltpu.make_async_copy(done_up.at[b], p_up.at[b], done_sem.at[2 * b]).wait()
        pltpu.make_async_copy(done_down.at[b], p_down.at[b], done_sem.at[2 * b + 1]).wait()


def finish(scale, decay, packed, *rest):
    f32 = lambda *shape: pltpu.VMEM(shape, jnp.float32)
    shape = lambda *dims: jax.ShapeDtypeStruct(dims, jnp.float32)
    any_spec = pl.BlockSpec(memory_space=pl.ANY)
    dma = pltpu.SemaphoreType.DMA
    return pl.pallas_call(
        functools.partial(finish_kernel, scale), name="finish",
        in_specs=[pl.BlockSpec(memory_space=pltpu.SMEM)] + [any_spec] * 9, out_specs=[any_spec] * 6,
        out_shape=[shape(2, BK, WIDTH), shape(2, WIDTH, BK), shape(2, BK, BK), shape(2, WIDTH, WIDTH),
                   shape(2, WIDTH, WIDTH), shape(2, BK, BK)],
        scratch_shapes=[
            f32(BLOCKS * BK, BK), f32(2, WIDTH, WIDTH), f32(2, WIDTH, WIDTH), f32(2, BK, BK), f32(2, BK, BK),
            f32(DEPTH, BK, WIDTH), f32(DEPTH, BK, WIDTH), f32(2, BK, BK), f32(2, BK, BK), f32(2, BK, BK), f32(2, BK, BK),
            f32(BK, WIDTH), f32(BK, BK), f32(2, BK, WIDTH), f32(2, WIDTH, BK),
            dma((PIECES,)), dma((6,)), dma((DEPTH,)), dma((DEPTH,)), dma((4,)), dma((4,))],
        cost_estimate=pl.CostEstimate(flops=16 * 10 ** 9, bytes_accessed=74 << 20, transcendentals=0),
        compiler_params=pltpu.CompilerParams(vmem_limit_bytes=VMEM_LIMIT),
    )(decay, packed, *rest)


def solution(mesh):
    axis_size = mesh.shape["data"]

    def local_step(tok, grad, w_up, w_down, a_up_old, s_up_old, a_down_old, s_down_old,
                   a_up_inv, s_up_inv, a_down_inv, s_down_inv, factor_decay):
        packed = statistics(tok, grad, w_up, w_down)
        scale = 1.0 / (tok.shape[0] * axis_size)
        return tuple(finish(scale, factor_decay.reshape(1), packed, a_up_old, s_up_old, a_down_old, s_down_old,
                            a_up_inv, s_up_inv, a_down_inv, s_down_inv))

    batch_spec = P("data", None)
    replicated = P()
    return jax.shard_map(local_step, mesh=mesh, in_specs=(batch_spec, batch_spec) + (replicated,) * 11,
                         out_specs=(replicated,) * 6, check_vma=False)
```

```python
import functools
import jax
import jax.numpy as jnp
from jax import lax
from jax.experimental import pallas as pl
from jax.experimental.pallas import tpu as pltpu
from jax.sharding import PartitionSpec as P

C0 = 0.7978845608028654
C1 = C0 * 0.044715
BK = 256
ROWS = 1024
SUB = 64
BLOCKS = 60
PIECE = 1024
PIECES = BLOCKS * BK // PIECE
RING = 8
CORE_RING = 3
SLOT_ROWS = 480
VMEM_LIMIT = 67043328
PAIRS = [(i, j) for i in range(4) for j in range(i, 4)]
GRAM_H0, GRAM_U0, GRAM_Q1 = 0, 10, 11
GRAM_H1, DOWN1 = 12, 22
GRAM_G1, UP1, GRAM_U1, GRAM_E1 = 26, 36, 40, 41
UP0, DOWN0, GRAM_G0 = 42, 46, 50
STAGES = 8
TIMES = (
    (10, 14, 16, 20, 23, 25, 26, 28, 29),
    (9, 12, 15, 17, 19, 21, 24, 26, 29),
    (8, 9, 13, 15, 17, 20, 23, 25, 27),
    (17, 18, 22, 24, 26, 28, 30, 32, 36),
    (17, 19, 21, 24, 27, 29, 32, 36, 39),
    (16, 17, 19, 22, 25, 27, 28, 32, 36),
    (24, 25, 27, 29, 31, 34, 37, 41, 43),
    (25, 27, 29, 32, 36, 39, 42, 46, 50),
    (29, 31, 33, 36, 40, 44, 48, 52, 53),
    (34, 36, 40, 44, 48, 52, 55, 58, 62),
    (33, 35, 39, 43, 45, 49, 52, 56, 58),
    (37, 39, 43, 46, 50, 53, 57, 60, 63),
    (44, 46, 49, 52, 53, 56, 59, 63, 64),
    (43, 45, 48, 51, 52, 56, 60, 64, 68),
    (49, 51, 52, 55, 57, 59, 63, 66, 70),
)


def dot(left, right):
    return jnp.dot(left, right, preferred_element_type=jnp.float32)


def dot_nt(left, right):
    return lax.dot_general(left, right, (((1,), (1,)), ((), ())), preferred_element_type=jnp.float32)


def blk(index):
    return pl.ds(index * BK, BK)


class Exchange:
    def __init__(self, acc, core_slots, slots, send, recv, free):
        self.core_slots = core_slots
        self.acc, self.slots, self.send, self.recv, self.free = acc, slots, send, recv, free
        me = lax.axis_index("data")
        self.me = me
        self.core = lax.rem(me, 2)
        self.plane = (lax.rem(me // 2, 2), lax.rem(me // 4, 2))
        self.z = me // 8
        flip = lambda bit, step: me + (1 - 2 * bit) * step
        self.core_peer = flip(self.core, 1)
        self.plane_peer = (flip(self.plane[0], 2), flip(self.plane[1], 4))
        base = lax.rem(me, 8)
        self.z_peer = [base + 8 * lax.rem(self.z + d, 4) for d in (1, 2, 3)]

    def barrier(self):
        sem = pltpu.get_barrier_semaphore()
        peers = [self.core_peer, *self.plane_peer, *self.z_peer]
        for peer in peers:
            pl.semaphore_signal(sem, inc=1, device_id=(peer,), device_id_type=pl.DeviceIdType.MESH)
        pl.semaphore_wait(sem, len(peers))

    def rows(self, start, size):
        return self.acc.at[pl.ds(pl.multiple_of(start, 16), size), :]

    def spots(self, piece, color):
        first, second = (0, 1) if color == 0 else (1, 0)
        base1 = piece * PIECE + self.core * 512 + color * 256
        bit1, bit2 = self.plane[first], self.plane[second]
        base2 = base1 + bit1 * 128
        base3 = base2 + bit2 * 64
        return first, second, bit1, bit2, base1, base2, base3

    def copies(self, piece, stage):
        ring = piece % RING
        slot = self.slots.at[ring]
        found = []

        def add(number, src, dst, peer, keep=None, got=None):
            sem = stage * 6 + number
            found.append((pltpu.make_async_remote_copy(
                src_ref=src, dst_ref=dst, send_sem=self.send.at[ring, sem], recv_sem=self.recv.at[ring, sem],
                device_id=(peer,), device_id_type=pl.DeviceIdType.MESH), keep, got, peer))

        top = piece * PIECE
        if stage == 0:
            got = self.core_slots.at[piece % CORE_RING]
            add(0, self.rows(top + (1 - self.core) * 512, 512), got, self.core_peer,
                (top + self.core * 512, 512), got)
        elif stage == 7:
            mine = self.rows(top + self.core * 512, 512)
            add(0, mine, mine, self.core_peer)
        for color in range(2):
            first, second, bit1, bit2, base1, base2, base3 = self.spots(piece, color)
            if stage == 1:
                got = slot.at[pl.ds(color * 128, 128), :]
                add(color, self.rows(base1 + (1 - bit1) * 128, 128), got, self.plane_peer[first], (base2, 128), got)
            elif stage == 2:
                got = slot.at[pl.ds(256 + color * 64, 64), :]
                add(color, self.rows(base2 + (1 - bit2) * 64, 64), got, self.plane_peer[second], (base3, 64), got)
            elif stage == 3:
                for d in range(3):
                    got = slot.at[pl.ds(384 + color * 48 + d * 16, 16), :]
                    peer_z = lax.rem(self.z + d + 1, 4)
                    add(color * 3 + d, self.rows(base3 + peer_z * 16, 16), got, self.z_peer[d],
                        (base3 + self.z * 16, 16), got)
            elif stage == 4:
                mine = self.rows(base3 + self.z * 16, 16)
                for d in range(3):
                    add(color * 3 + d, mine, mine, self.z_peer[d])
            elif stage == 5:
                mine = self.rows(base3, 64)
                add(color, mine, mine, self.plane_peer[second])
            elif stage == 6:
                mine = self.rows(base2, 128)
                add(color, mine, mine, self.plane_peer[first])
        return found

    def credits(self, piece, stage):
        colors = 1 if stage == 0 else 2
        return [self.free.at[piece % RING, 2 * stage + color] for color in range(colors)]

    def start(self, piece, stage):
        found = self.copies(piece, stage)
        back = 0 if stage == 2 else STAGES - 1 - stage
        if stage == 2 or STAGES // 2 <= stage < STAGES - 1:
            credits = self.credits(piece, back)
            peers = 1 if back == 0 else len(found) // len(credits)
            for credit in credits:
                pl.semaphore_wait(credit, peers)
        for copy, *_ in found:
            copy.start()

    def finish(self, piece, stage):
        found = self.copies(piece, stage)
        for copy, *_ in found:
            copy.wait()
        if stage < STAGES // 2:
            for _, keep, got, _ in found:
                self.rows(*keep)[...] += got[...]
            credits = self.credits(piece, stage)
            per = len(found) // len(credits)
            for number, (_, _, _, peer) in enumerate(found):
                pl.semaphore_signal(credits[number // per], inc=1, device_id=(peer,),
                                    device_id_type=pl.DeviceIdType.MESH)

    def slot_of_time(self, events):
        for piece, stage in events:
            if stage > 0:
                self.finish(piece, stage - 1)
            if stage < STAGES:
                self.start(piece, stage)


def cdf_of(pre):
    square = pre * pre
    return square, 0.5 * jnp.tanh(pre * (C1 * square + C0)) + 0.5


def slope_of(pre, square, cdf):
    return cdf * (((1.0 - cdf) * pre) * (6.0 * C1 * square + 2.0 * C0) + 1.0)


def produce_forward(col, u, w_ref, z_ref, h_ref):
    z_ref[...] = dot(u[...], w_ref[:, blk(col)]).astype(jnp.bfloat16)
    for row in range(0, ROWS, SUB):
        pre = z_ref[row:row + SUB, :].astype(jnp.float32)
        _, cdf = cdf_of(pre)
        h_ref[row:row + SUB, blk(col)] = (pre * cdf).astype(jnp.bfloat16)


def produce_both(col, u, w_ref, q, wd_ref, z_ref, d_ref, h_ref, g, off):
    z_ref[...] = dot(u[...], w_ref[:, blk(col)]).astype(jnp.bfloat16)
    d_ref[...] = dot_nt(q[...], wd_ref[blk(col), :]).astype(jnp.bfloat16)
    for row in range(0, ROWS, SUB):
        pre = z_ref[row:row + SUB, :].astype(jnp.float32)
        d_hidden = d_ref[row:row + SUB, :].astype(jnp.float32)
        square, cdf = cdf_of(pre)
        h_ref[row:row + SUB, blk(col)] = (pre * cdf).astype(jnp.bfloat16)
        g[pl.ds(off + row, SUB), blk(col)] = (d_hidden * slope_of(pre, square, cdf)).astype(jnp.bfloat16)


def kernel(tok_hbm, grad_hbm, w_up_hbm, w_down_hbm, out_hbm,
           acc, core_slots, slots, tok, grad, mid, g1, w_up, w_down, z0, z1, d0, d1, h_ref, t_ref,
           send, recv, free, tok_sem, grad_sem, w_sem, out_sem):
    tiles = tok.shape[0] // ROWS
    w_copies = [pltpu.make_async_copy(w_up_hbm, w_up, w_sem.at[0]),
                pltpu.make_async_copy(w_down_hbm, w_down, w_sem.at[1])]

    def tile_copies(i):
        rows = pl.ds(pl.multiple_of(i * ROWS, ROWS), ROWS)
        return (pltpu.make_async_copy(tok_hbm.at[rows, :], tok.at[rows, :], tok_sem.at[i]),
                pltpu.make_async_copy(grad_hbm.at[rows, :], grad.at[rows, :], grad_sem.at[i]))

    for copy in w_copies:
        copy.start()
    for i in range(tiles):
        for copy in tile_copies(i):
            copy.start()
    exchange = Exchange(acc, core_slots, slots, send, recv, free)
    exchange.barrier()

    @pl.loop(0, BLOCKS)
    def _(n):
        acc[pl.ds(pl.multiple_of(n * BK, BK), BK), :] = jnp.zeros((BK, BK), jnp.float32)

    for copy in w_copies:
        copy.wait()
    zs, ds_ = (z0, z1), (d0, d1)

    def out_copy(piece):
        rows = pl.ds(piece * PIECE, PIECE)
        return pltpu.make_async_copy(acc.at[rows, :], out_hbm.at[rows, :], out_sem.at[piece])

    def events_at(now):
        return [(piece, stage) for piece in range(PIECES) for stage in range(STAGES + 1) if TIMES[piece][stage] == now]

    def fire(events):
        if events:
            exchange.slot_of_time(events)
            for piece, stage in events:
                if stage == STAGES:
                    out_copy(piece).start()

    def hooks(i, first):
        for n in range(tiles):
            events = events_at(first + n)
            if events:
                pl.when(i == n)(functools.partial(fire, events))

    def add_to(slot, value):
        acc[blk(slot), :] += value

    def gram_column(first, col, x):
        for i in range(col + 1):
            add_to(first + PAIRS.index((i, col)), dot(t_ref[blk(i), :], x(col)))

    def views(i):
        off = pl.multiple_of(i * ROWS, ROWS)
        rows = pl.ds(off, ROWS)
        return off, tok.at[rows, :], grad.at[rows, :], mid.at[rows, :]

    @pl.loop(0, tiles)
    def _(i):
        off, u, q, nxt = views(i)
        for copy in tile_copies(i):
            copy.wait()
        hx = lambda col: h_ref[:, blk(col)]

        def produce(col):
            produce_forward(col, u, w_up.at[0], zs[col % 2], h_ref)
            t_ref[blk(col), :] = h_ref[:, blk(col)].T

        small = t_ref.at[blk(3), :]
        produce(0)
        small[...] = u[...].T
        add_to(GRAM_U0, dot(small[...], u[...]))
        produce(1)
        gram_column(GRAM_H0, 0, hx)
        small[...] = q[...].T
        add_to(GRAM_Q1, dot(small[...], q[...]))
        produce(2)
        gram_column(GRAM_H0, 1, hx)
        produce(3)
        gram_column(GRAM_H0, 2, hx)
        nxt[...] = dot(h_ref[...], w_down[0]).astype(jnp.bfloat16)
        gram_column(GRAM_H0, 3, hx)

    @pl.loop(0, tiles)
    def _(i):
        hooks(i, 8)
        off, _, q, u = views(i)
        hx = lambda col: h_ref[:, blk(col)]

        def produce(col):
            produce_both(col, u, w_up.at[1], q, w_down.at[1], zs[col % 2], ds_[col % 2], h_ref, g1, off)
            t_ref[blk(col), :] = h_ref[:, blk(col)].T

        def consume(col):
            gram_column(GRAM_H1, col, hx)
            add_to(DOWN1 + col, dot(t_ref[blk(col), :], q[...]))

        produce(0)
        for col in range(1, 4):
            produce(col)
            consume(col - 1)
        consume(3)

    @pl.loop(0, tiles)
    def _(i):
        hooks(i, 16)
        off, _, _, u = views(i)
        rows = pl.ds(off, ROWS)
        gx = lambda col: g1[rows, blk(col)]
        small = h_ref.at[blk(0), :]
        small[...] = u[...].T
        add_to(GRAM_U1, dot(small[...], u[...]))
        for col in range(4):
            t_ref[blk(col), :] = gx(col).T
            add_to(UP1 + col, dot(small[...], gx(col)))
            gram_column(GRAM_G1, col, gx)
        u[...] = dot_nt(g1[rows, :], w_up[1]).astype(jnp.bfloat16)
        small[...] = u[...].T
        add_to(GRAM_E1, dot(small[...], u[...]))

    @pl.loop(0, tiles)
    def _(i):
        hooks(i, 24)
        off, u, _, q = views(i)
        rows = pl.ds(off, ROWS)

        def produce(col):
            produce_both(col, u, w_up.at[0], q, w_down.at[0], zs[col % 2], ds_[col % 2], h_ref, g1, off)
            t_ref[blk(col % 3), :] = h_ref[:, blk(col)].T

        def consume(col):
            add_to(UP0 + col, dot(small[...], g1[rows, blk(col)]))
            add_to(DOWN0 + col, dot(t_ref[blk(col % 3), :], q[...]))

        small = t_ref.at[blk(3), :]
        small[...] = u[...].T
        produce(0)
        for col in range(1, 4):
            produce(col)
            consume(col - 1)
        consume(3)

    def gram_row(row, now):
        halves = 2 if row < 2 else 1
        per = tiles // halves
        for half in range(halves):
            fire(events_at(now + half))

            @pl.loop(half * per, (half + 1) * per)
            def _(i):
                rows = pl.ds(pl.multiple_of(i * ROWS, ROWS), ROWS)
                small = t_ref.at[blk(0), :]
                small[...] = g1[rows, blk(row)].T
                for col in range(row, 4):
                    add_to(GRAM_G0 + PAIRS.index((row, col)), dot(small[...], g1[rows, blk(col)]))
        return now + halves

    now = 32
    for row in range(4):
        now = gram_row(row, now)
    while now <= max(times[-1] for times in TIMES):
        fire(events_at(now))
        now += 1
    for piece in range(PIECES):
        out_copy(piece).wait()


def statistics(tok, grad, w_up, w_down):
    rows = tok.shape[0]
    tiles = rows // ROWS
    bf = lambda *shape: pltpu.VMEM(shape, jnp.bfloat16)
    any_spec = pl.BlockSpec(memory_space=pl.ANY)
    dma = pltpu.SemaphoreType.DMA
    return pl.pallas_call(
        kernel, name="statistics", in_specs=[any_spec] * 4, out_specs=any_spec,
        out_shape=jax.ShapeDtypeStruct((BLOCKS * BK, BK), jnp.float32),
        scratch_shapes=[
            pltpu.VMEM((BLOCKS * BK, BK), jnp.float32), pltpu.VMEM((CORE_RING, 512, BK), jnp.float32),
            pltpu.VMEM((RING, SLOT_ROWS, BK), jnp.float32),
            bf(rows, BK), bf(rows, BK), bf(rows, BK), bf(rows, 4 * BK), bf(*w_up.shape), bf(*w_down.shape),
            bf(ROWS, BK), bf(ROWS, BK), bf(ROWS, BK), bf(ROWS, BK),
            bf(ROWS, 4 * BK), bf(4 * BK, ROWS),
            dma((RING, 6 * STAGES)), dma((RING, 6 * STAGES)),
            pltpu.SemaphoreType.REGULAR((RING, STAGES)), dma((tiles,)), dma((tiles,)), dma((2,)), dma((PIECES,))],
        cost_estimate=pl.CostEstimate(flops=100 * 10 ** 9, bytes_accessed=30 << 20, transcendentals=0),
        compiler_params=pltpu.CompilerParams(vmem_limit_bytes=VMEM_LIMIT, collective_id=0, has_side_effects=True),
    )(tok, grad, w_up, w_down)


def precise(left, right):
    return jnp.dot(left, right, precision=lax.Precision.HIGHEST, preferred_element_type=jnp.float32)


WIDTH = 4 * BK
STEPS = 16
DEPTH = 4


def finish_kernel(scale, decay, packed_hbm, a_up_old, s_up_old, a_down_old, s_down_old,
                  a_up_inv, s_up_inv, a_down_inv, s_down_inv,
                  p_up, p_down, a_up_new, s_up_new, a_down_new, s_down_new,
                  packed, wide_up, wide_down, small_up, small_down, old_ring, new_ring,
                  old_a, old_s, new_a, new_s, mid_up, mid_down, done_up, done_down,
                  pk_sem, inv_sem, old_sem, new_sem, small_sem, done_sem):
    keep = decay[0]
    fresh = (1.0 - decay[0]) * scale

    def pk_copy(piece):
        rows = pl.ds(piece * PIECE, PIECE)
        return pltpu.make_async_copy(packed_hbm.at[rows, :], packed.at[rows, :], pk_sem.at[piece])

    inv_copies = [pltpu.make_async_copy(a_up_inv, small_up, inv_sem.at[0]),
                  pltpu.make_async_copy(s_down_inv, small_down, inv_sem.at[1])]
    for b in range(2):
        inv_copies.append(pltpu.make_async_copy(s_up_inv.at[b], wide_up.at[b], inv_sem.at[2 + 2 * b]))
        inv_copies.append(pltpu.make_async_copy(a_down_inv.at[b], wide_down.at[b], inv_sem.at[3 + 2 * b]))
    grams = [(a_down_old, a_down_new, 0, GRAM_H0), (a_down_old, a_down_new, 1, GRAM_H1),
             (s_up_old, s_up_new, 1, GRAM_G1), (s_up_old, s_up_new, 0, GRAM_G0)]

    def old_copy(step):
        old, _, b, _ = grams[step // 4]
        return pltpu.make_async_copy(old.at[b, pl.ds(step % 4 * BK, BK), :], old_ring.at[step % DEPTH],
                                     old_sem.at[step % DEPTH])

    def new_copy(step):
        _, new, b, _ = grams[step // 4]
        return pltpu.make_async_copy(new_ring.at[step % DEPTH], new.at[b, pl.ds(step % 4 * BK, BK), :],
                                     new_sem.at[step % DEPTH])

    small_ins = [pltpu.make_async_copy(a_up_old, old_a, small_sem.at[0]),
                 pltpu.make_async_copy(s_down_old, old_s, small_sem.at[1])]
    small_outs = [pltpu.make_async_copy(new_a, a_up_new, small_sem.at[2]),
                  pltpu.make_async_copy(new_s, s_down_new, small_sem.at[3])]
    waited = set()

    def block(n):
        piece = n * BK // PIECE
        if piece not in waited:
            waited.add(piece)
            pk_copy(piece).wait()
        return packed[blk(n), :]

    def update(step):
        _, _, _, first = grams[step // 4]
        row = step % 4
        old_copy(step).wait()
        if step >= DEPTH:
            new_copy(step - DEPTH).wait()
        for col in range(4):
            pair = (min(row, col), max(row, col))
            value = block(first + PAIRS.index(pair))
            value = value if row <= col else value.T
            new_ring[step % DEPTH, :, blk(col)] = keep * old_ring[step % DEPTH, :, blk(col)] + fresh * value
        new_copy(step).start()
        if step + DEPTH < STEPS:
            old_copy(step + DEPTH).start()

    for step in range(DEPTH):
        old_copy(step).start()
    loads = [[pk_copy(n) for n in (0, 1, 2, 5, 6)] + [inv_copies[5], inv_copies[1]],
             [pk_copy(n) for n in (3, 4)] + [inv_copies[4], inv_copies[0]],
             [pk_copy(n) for n in (9, 10, 7, 8)],
             [inv_copies[3]] + [pk_copy(n) for n in (11, 12, 13, 14)],
             small_ins + [inv_copies[2]]]

    def load_next():
        if loads:
            for copy in loads.pop(0):
                copy.start()

    load_next()

    def chain_up(b, first):
        if b == 1:
            inv_copies[0].wait()
        for col in range(4):
            mid_up[:, blk(col)] = precise(small_up[b], block(first + col) * scale)

    def chain_up_end(b, col):
        if col == 0:
            inv_copies[2 + 2 * b].wait()
        done_up[b, :, blk(col)] = precise(mid_up[...], wide_up[b, :, blk(col)])
        if col == 3:
            pltpu.make_async_copy(done_up.at[b], p_up.at[b], done_sem.at[2 * b]).start()

    def chain_down(b, first, row):
        if row == 0:
            inv_copies[3 + 2 * b].wait()
            if b == 1:
                inv_copies[1].wait()
            for n in range(4):
                block(first + n)
        mid_down[...] = precise(wide_down[b, blk(row), :], packed[first * BK:(first + 4) * BK, :] * scale)
        done_down[b, blk(row), :] = precise(mid_down[...], small_down[b])
        if row == 3:
            pltpu.make_async_copy(done_down.at[b], p_down.at[b], done_sem.at[2 * b + 1]).start()

    for step in range(4):
        update(step)
        load_next()
    for n in range(4):
        chain_down(1, DOWN1, n)
        update(4 + n)
    chain_up(1, UP1)
    for n in range(4):
        chain_up_end(1, n)
        update(8 + n)
    for n in range(4):
        chain_down(0, DOWN0, n)
        update(12 + n)
    for copy in small_ins:
        copy.wait()
    for b, first in ((0, GRAM_U0), (1, GRAM_U1)):
        new_a[b] = keep * old_a[b] + fresh * block(first)
    for b, first in ((0, GRAM_E1), (1, GRAM_Q1)):
        new_s[b] = keep * old_s[b] + fresh * block(first)
    for copy in small_outs:
        copy.start()
    chain_up(0, UP0)
    for n in range(4):
        chain_up_end(0, n)
    for step in range(STEPS - DEPTH, STEPS):
        new_copy(step).wait()
    for copy in small_outs:
        copy.wait()
    for b in range(2):
        pltpu.make_async_copy(done_up.at[b], p_up.at[b], done_sem.at[2 * b]).wait()
        pltpu.make_async_copy(done_down.at[b], p_down.at[b], done_sem.at[2 * b + 1]).wait()


def finish(scale, decay, packed, *rest):
    f32 = lambda *shape: pltpu.VMEM(shape, jnp.float32)
    shape = lambda *dims: jax.ShapeDtypeStruct(dims, jnp.float32)
    any_spec = pl.BlockSpec(memory_space=pl.ANY)
    dma = pltpu.SemaphoreType.DMA
    return pl.pallas_call(
        functools.partial(finish_kernel, scale), name="finish",
        in_specs=[pl.BlockSpec(memory_space=pltpu.SMEM)] + [any_spec] * 9, out_specs=[any_spec] * 6,
        out_shape=[shape(2, BK, WIDTH), shape(2, WIDTH, BK), shape(2, BK, BK), shape(2, WIDTH, WIDTH),
                   shape(2, WIDTH, WIDTH), shape(2, BK, BK)],
        scratch_shapes=[
            f32(BLOCKS * BK, BK), f32(2, WIDTH, WIDTH), f32(2, WIDTH, WIDTH), f32(2, BK, BK), f32(2, BK, BK),
            f32(DEPTH, BK, WIDTH), f32(DEPTH, BK, WIDTH), f32(2, BK, BK), f32(2, BK, BK), f32(2, BK, BK), f32(2, BK, BK),
            f32(BK, WIDTH), f32(BK, BK), f32(2, BK, WIDTH), f32(2, WIDTH, BK),
            dma((PIECES,)), dma((6,)), dma((DEPTH,)), dma((DEPTH,)), dma((4,)), dma((4,))],
        cost_estimate=pl.CostEstimate(flops=16 * 10 ** 9, bytes_accessed=74 << 20, transcendentals=0),
        compiler_params=pltpu.CompilerParams(vmem_limit_bytes=VMEM_LIMIT),
    )(decay, packed, *rest)


def solution(mesh):
    axis_size = mesh.shape["data"]

    def local_step(tok, grad, w_up, w_down, a_up_old, s_up_old, a_down_old, s_down_old,
                   a_up_inv, s_up_inv, a_down_inv, s_down_inv, factor_decay):
        packed = statistics(tok, grad, w_up, w_down)
        scale = 1.0 / (tok.shape[0] * axis_size)
        return tuple(finish(scale, factor_decay.reshape(1), packed, a_up_old, s_up_old, a_down_old, s_down_old,
                            a_up_inv, s_up_inv, a_down_inv, s_down_inv))

    batch_spec = P("data", None)
    replicated = P()
    return jax.shard_map(local_step, mesh=mesh, in_specs=(batch_spec, batch_spec) + (replicated,) * 11,
                         out_specs=(replicated,) * 6, check_vma=False)
```
